128 devices in a mesh: tri: 128 (over z, y, x, core).
Axes of the slice: x: 4, y: 4, z: 4, core: 2. Of those that a mesh axis runs over, the one named last changes fastest.
Arguments:
- amplitudes: bfloat16 [128, 2816, 1408], P('tri'), as said below
- factors: bfloat16 [22528, 1280], P('tri'), may hold values from -2.5 to 2.5
- occ_energy: float32 [44], replicated, may hold values from -3 to -0.5
- virt_energy: float32 [512], replicated, may hold values from 0.2 to 6
Outputs:
- new_amplitudes: float32 [128, 2816, 1408], P('tri')
The draws below stay inside these ranges and needn't reach their ends.
Inputs may be any that keep to these rules, and one draw needn't show every extreme that they name: `amplitudes`: the matrix T assembled from the tiles is symmetric.
All inputs are finite; a program needn't handle non-finite values.
Results may differ from the reference program's by a relative error of at most 0.0069.
Values may be sent and summed in bfloat16 or wider, within the bound.
No kernel may reach another device: no remote copies, remote signals or barrier semaphores. Data moves between devices by JAX's collectives and lax.ppermute only.
A program may use at most 128 MiB of HBM per device.

```python
import math
import jax
import jax.numpy as jnp
from jax import lax

OCC = 44
VIRT = 512
NAUX = 1280
STRIPES = 8
OV = 22528
ROWS = 176
BAND = 16
N_TRI = 128


def draw_amplitudes(key, part):
    scale = 0.7 / OV ** 0.5
    indices = jnp.arange(N_TRI, dtype=jnp.int32)

    def block_row(upper):

        def one_block(lower):
            small = jnp.minimum(upper, lower)
            large = jnp.maximum(upper, lower)
            subkey = jax.random.fold_in(key, small * N_TRI + large)
            values = jax.random.normal(subkey, (ROWS, ROWS), jnp.float32)
            values = jnp.where(upper == lower, (values + values.T) * 0.70710678, values)
            values = jnp.where(upper > lower, values.T, values)
            return (values * scale).astype(jnp.bfloat16)
        return jax.vmap(one_block)(indices)
    blocks = lax.map(block_row, indices)
    blocks = blocks.reshape(STRIPES, BAND, STRIPES, BAND, ROWS, ROWS)
    blocks = blocks.transpose(0, 3, 1, 4, 2, 5)
    return blocks.reshape(N_TRI, BAND * ROWS, STRIPES * ROWS)


def block_levels(rng, extent, cuts, least, high):
    loudness = 1.0
    for dim, parts in cuts:
        heights = jax.random.uniform(jax.random.fold_in(jax.random.fold_in(rng, 6), dim), (parts,), jnp.float32, least / len(cuts), high / len(cuts))
        loudness = loudness * jnp.repeat(jnp.exp(heights), extent[dim] // parts).reshape((-1,) + (1,) * (len(extent) - 1 - dim))
    return loudness


def centred(rng, dims, scale, bound, split=(), kind=jnp.bfloat16):
    level = block_levels(rng, dims, split, -0.22, 0.18) if split else 1.0
    array = jax.random.normal(rng, dims, jnp.float32) * scale * level
    return jnp.minimum(jnp.maximum(array, -bound), bound).astype(kind)


def setup_inputs(seed: int = 0) -> dict:
    arg_keys = jax.random.split(jax.random.key(seed), 5)
    return {
        "amplitudes": draw_amplitudes(jax.random.fold_in(arg_keys[4], 71), 0),
        "factors": centred(arg_keys[1], (OV, NAUX), 0.35, 2.5, ((0, 128),)),
        "occ_energy": jnp.clip(jax.random.uniform(arg_keys[2], (OCC,), jnp.float32, -3.0, -0.5), -3.0, -0.5),
        "virt_energy": jnp.clip(jnp.exp(jax.random.uniform(arg_keys[3], (VIRT,), jnp.float32, math.log(0.2), math.log(6.0))), 0.2, 6.0),
    }


def reference(amplitudes, factors, occ_energy, virt_energy):
    pair_energy = (virt_energy[None, :] - occ_energy[:, None]).reshape(OCC * VIRT)
    column_sets = factors.reshape(STRIPES, BAND, ROWS, NAUX).transpose(1, 0, 2, 3).reshape(BAND, STRIPES * ROWS, NAUX)
    tiles = amplitudes.reshape(STRIPES, BAND, BAND * ROWS, STRIPES * ROWS)

    def band_images(tile_row):
        def accumulate(total, pair):
            return total + jnp.dot(pair[0], pair[1], preferred_element_type=jnp.float32), None

        start = jnp.zeros((BAND * ROWS, NAUX), jnp.float32)
        total, unused = lax.scan(accumulate, start, (tile_row, column_sets))
        return total

    images = lax.map(band_images, tiles).reshape(OV, NAUX) + factors.astype(jnp.float32)
    dressed = images.astype(jnp.bfloat16)
    dressed_bands = dressed.reshape(STRIPES, BAND * ROWS, NAUX)
    dressed_sets = dressed.reshape(STRIPES, BAND, ROWS, NAUX).transpose(1, 0, 2, 3).reshape(BAND, STRIPES * ROWS, NAUX)
    energy_bands = pair_energy.reshape(STRIPES, BAND * ROWS)
    energy_sets = pair_energy.reshape(STRIPES, BAND, ROWS).transpose(1, 0, 2).reshape(BAND, STRIPES * ROWS)

    def one_tile(index):
        stripe = index // BAND
        column = index % BAND
        inner = jnp.dot(dressed_bands[stripe], dressed_sets[column].T, preferred_element_type=jnp.float32)
        return -inner / (energy_bands[stripe][:, None] + energy_sets[column][None, :])

    return lax.map(one_tile, jnp.arange(N_TRI, dtype=jnp.int32))
```

```python
import functools
import jax
import jax.numpy as jnp
from jax import lax
from jax.experimental import pallas as pl
from jax.experimental.pallas import tpu as pltpu
from jax.sharding import PartitionSpec as P

AXIS = "tri"
DEVICES = 128
LIMIT = 56 * 2**20


def place(index):
    return index // 32, index // 8 % 4, index // 2 % 4, index % 2


def index_of(z, y, x, core):
    return ((z % 4 * 4 + y % 4) * 4 + x % 4) * 2 + core


def send(value, dz=0, y_flip=0, dx=0, core_flip=0):
    pairs = []
    for source in range(DEVICES):
        z, y, x, core = place(source)
        pairs.append((source, index_of(z + dz, y ^ y_flip, x + dx, core ^ core_flip)))
    return lax.ppermute(value, AXIS, pairs)


def split_rows(rows):
    return rows - rows // 32 * 16


def gather_ring(own, along, y_flip):
    rows = own.shape[0]
    low = split_rows(rows)
    up, down = {along: 1}, {along: -1}
    partner = send(own, y_flip=y_flip)
    left = send(own, **up)
    right = send(own, **down)
    from_left = send(jnp.concatenate([partner, left[:low]], 0), **up)
    from_right = send(jnp.concatenate([partner, right[low:]], 0), **down)
    third_low = send(from_left[:low], **up)
    third_high = send(from_right[low:rows], **down)
    return (own, left, right, partner, from_left, from_right, third_low, third_high)


def swap_cores(pieces):
    first = jnp.concatenate(pieces[:4], 0)
    second = jnp.concatenate(pieces[4:6], 0)
    third = jnp.concatenate(pieces[6:], 0)
    return tuple(send(buffer, core_flip=1) for buffer in (first, second, third))


def ring_moves(rows):
    low = split_rows(rows)
    high = rows - low
    return [
        (0, 0, rows, 0, 0, 0),
        (1, 0, rows, 3, 0, 0),
        (2, 0, rows, 1, 0, 0),
        (3, 0, rows, 0, 1, 0),
        (4, 0, rows, 3, 1, 0),
        (4, rows, low, 2, 0, 0),
        (5, 0, rows, 1, 1, 0),
        (5, rows, high, 2, 0, low),
        (6, 0, low, 2, 1, 0),
        (7, 0, high, 2, 1, low),
    ]


def joined_moves(rows):
    low = split_rows(rows)
    starts = [(0, 0), (0, rows), (0, 2 * rows), (0, 3 * rows), (1, 0), (1, rows + low), (2, 0), (2, low)]
    moves = []
    for piece, row, count, step, partner, at in ring_moves(rows):
        buffer, base = starts[piece]
        moves.append((buffer, base + row, count, step, partner, at))
    return moves


def position():
    index = lax.axis_index(AXIS)
    z = index // 32
    upper = lax.rem(index // 16, 2)
    lower = lax.rem(index // 8, 2)
    x = lax.rem(index // 2, 4)
    core = lax.rem(index, 2)
    return z, upper, lower, x, core


def band_slot(step, partner, flip):
    z, upper, lower, x, core = position()
    other_row = (1 - lower) if partner else lower
    other_core = (1 - core) if flip else core
    return other_row * 8 + lax.rem(x + step, 4) * 2 + other_core


def set_slot(step, partner):
    z, upper, lower, x, core = position()
    return lax.rem(z + step, 4) * 2 + ((1 - upper) if partner else upper)


def copies_of(rows, refs, moves, slot, target, sems, first):
    out = []
    for number, (piece, row, count, step, partner, at) in enumerate(moves):
        begin = pl.multiple_of(slot(step, partner) * rows + at, 16)
        out.append(
            pltpu.make_async_copy(
                refs[piece].at[pl.ds(row, count), :],
                target.at[pl.ds(begin, count), :],
                sems.at[first + number],
            )
        )
    return out


def band_copies(rows, refs, target, sems, first=0):
    own = copies_of(
        rows, refs[:8], ring_moves(rows), lambda s, p: band_slot(s, p, 0), target, sems, first
    )
    other = copies_of(
        rows,
        refs[8:11],
        joined_moves(rows),
        lambda s, p: band_slot(s, p, 1),
        target,
        sems,
        first + 10,
    )
    return own + other


def set_copies(rows, refs, target, sems, first=0):
    return copies_of(rows, refs, ring_moves(rows), set_slot, target, sems, first)


def transposed_kernel(rows, *refs):
    pieces, (tile, far_low, far_high, near), (gathered, total, sems) = (
        refs[:11],
        refs[11:15],
        refs[15:],
    )
    step = pl.program_id(0)
    depth = tile.shape[1]
    z, upper, lower, x, core = position()

    @pl.when(step == 0)
    def _():
        copies = band_copies(rows, pieces, gathered, sems)
        for copy in copies:
            copy.start()
        for copy in copies:
            copy.wait()

    block = gathered[pl.ds(pl.multiple_of(step * depth, 16), depth), :]
    term = lax.dot_general(
        tile[0], block, (((0,), (0,)), ((), ())), preferred_element_type=jnp.float32
    )

    @pl.when(step == 0)
    def _():
        total[...] = term

    @pl.when(step > 0)
    def _():
        total[...] += term

    @pl.when(step == pl.num_programs(0) - 1)
    def _():
        def chunk(shift):
            return total[pl.ds(pl.multiple_of(lax.rem(z + shift, 4) * 2 * rows, 16), 2 * rows), :]

        far = chunk(2)
        far_low[...] = far[:rows].astype(far_low.dtype)
        far_high[...] = far[rows:].astype(far_high.dtype)
        near[: 2 * rows, :] = chunk(0)
        near[2 * rows : 4 * rows, :] = chunk(1)
        near[4 * rows :, :] = chunk(3)


def straight_kernel(rows, *refs):
    pieces, (tile, leaving, keeping), (gathered, product, sems) = refs[:8], refs[8:11], refs[11:]
    step = pl.program_id(0)
    z, upper, lower, x, core = position()

    @pl.when(step == 0)
    def _():
        copies = set_copies(rows, pieces, gathered, sems)
        for copy in copies:
            copy.start()
        for copy in copies:
            copy.wait()

    product[...] = jnp.dot(tile[0], gathered[...], preferred_element_type=jnp.float32)
    apart = lax.rem(lax.rem(step, 4) - x + 4, 4)
    begin = pl.multiple_of((apart * 2 + step // 4) * rows, 16)
    mine = pl.multiple_of(core * rows, 16)
    other = pl.multiple_of((1 - core) * rows, 16)
    leaving[pl.ds(begin, rows), :] = product[pl.ds(other, rows), :].astype(leaving.dtype)
    keeping[pl.ds(begin, rows), :] = product[pl.ds(mine, rows), :]


def outer_kernel(rows, *refs):
    pieces, (row_energy, column_energy, out), (band, column_set, sems) = (
        refs[:19],
        refs[19:22],
        refs[22:],
    )
    step = pl.program_id(0)
    depth = out.shape[1]

    @pl.when(step == 0)
    def _():
        copies = band_copies(rows, pieces[:11], band, sems)
        copies += set_copies(rows, pieces[11:], column_set, sems, 20)
        for copy in copies:
            copy.start()
        for copy in copies:
            copy.wait()

    block = band[pl.ds(pl.multiple_of(step * depth, 16), depth), :]
    inner = lax.dot_general(
        block, column_set[...], (((1,), (1,)), ((), ())), preferred_element_type=jnp.float32
    )
    out[0] = -inner / (row_energy[...] + column_energy[...])


def anywhere(count):
    return [pl.BlockSpec(memory_space=pl.ANY)] * count


def params():
    return pltpu.CompilerParams(dimension_semantics=("arbitrary",), vmem_limit_bytes=LIMIT)


def cost(rows, columns, depth):
    return pl.CostEstimate(
        flops=2 * rows * columns * depth,
        bytes_accessed=2 * rows * depth + 4 * rows * columns,
        transcendentals=0,
    )


def transposed_product(tile, pieces, steps=4):
    rows, width = pieces[0].shape
    depth, columns = tile.shape[1:]
    part = depth // steps
    return pl.pallas_call(
        functools.partial(transposed_kernel, rows),
        grid=(steps,),
        in_specs=anywhere(11) + [pl.BlockSpec((1, part, columns), lambda i: (0, i, 0))],
        out_specs=[
            pl.BlockSpec((rows, width), lambda i: (0, 0)),
            pl.BlockSpec((rows, width), lambda i: (0, 0)),
            pl.BlockSpec((6 * rows, width), lambda i: (0, 0)),
        ],
        out_shape=[
            jax.ShapeDtypeStruct((rows, width), jnp.bfloat16),
            jax.ShapeDtypeStruct((rows, width), jnp.bfloat16),
            jax.ShapeDtypeStruct((6 * rows, width), jnp.float32),
        ],
        scratch_shapes=[
            pltpu.VMEM((depth, width), jnp.bfloat16),
            pltpu.VMEM((columns, width), jnp.float32),
            pltpu.SemaphoreType.DMA((20,)),
        ],
        compiler_params=params(),
        cost_estimate=cost(columns, width, depth),
        name="transposed_product",
    )(*pieces, tile)


def straight_product(tile, pieces):
    rows, width = pieces[0].shape
    height, depth = tile.shape[1:]
    return pl.pallas_call(
        functools.partial(straight_kernel, rows),
        grid=(8,),
        in_specs=anywhere(8) + [pl.BlockSpec((1, 2 * rows, depth), lambda i: (0, i, 0))],
        out_specs=[
            pl.BlockSpec((height // 2, width), lambda i: (0, 0)),
            pl.BlockSpec((height // 2, width), lambda i: (0, 0)),
        ],
        out_shape=[
            jax.ShapeDtypeStruct((height // 2, width), jnp.bfloat16),
            jax.ShapeDtypeStruct((height // 2, width), jnp.float32),
        ],
        scratch_shapes=[
            pltpu.VMEM((depth, width), jnp.bfloat16),
            pltpu.VMEM((2 * rows, width), jnp.float32),
            pltpu.SemaphoreType.DMA((10,)),
        ],
        compiler_params=params(),
        cost_estimate=cost(height, width, depth),
        name="straight_product",
    )(*pieces, tile)


def outer_product(band, column_set, row_energy, column_energy, steps=8):
    rows, width = column_set[0].shape
    height, columns = 16 * rows, 8 * rows
    part = height // steps
    return pl.pallas_call(
        functools.partial(outer_kernel, rows),
        grid=(steps,),
        in_specs=anywhere(19)
        + [
            pl.BlockSpec((part, 1), lambda i: (i, 0)),
            pl.BlockSpec((1, columns), lambda i: (0, 0)),
        ],
        out_specs=pl.BlockSpec((1, part, columns), lambda i: (0, i, 0)),
        out_shape=jax.ShapeDtypeStruct((1, height, columns), jnp.float32),
        scratch_shapes=[
            pltpu.VMEM((height, width), jnp.bfloat16),
            pltpu.VMEM((columns, width), jnp.bfloat16),
            pltpu.SemaphoreType.DMA((30,)),
        ],
        compiler_params=params(),
        cost_estimate=cost(height, columns, width),
        name="outer_product",
    )(*band, *column_set, row_energy[:, None], column_energy[None, :])


def reduce_ring(far_low, far_high, own, after, before, along, y_flip, is_upper):
    rows = far_low.shape[0]
    up, down = {along: 1}, {along: -1}
    from_left = send(far_low, **up).astype(jnp.float32)
    from_right = send(far_high, **down).astype(jnp.float32)
    forward = jnp.concatenate([after[:rows] + from_left, after[rows:]], 0)
    backward = jnp.concatenate([before[:rows], before[rows:] + from_right], 0)
    left = send(forward.astype(jnp.bfloat16), **up).astype(jnp.float32)
    right = send(backward.astype(jnp.bfloat16), **down).astype(jnp.float32)
    total = own + left + right
    mine = jnp.where(is_upper, total[rows:], total[:rows])
    other = jnp.where(is_upper, total[:rows], total[rows:])
    return mine + send(other.astype(jnp.bfloat16), y_flip=y_flip).astype(jnp.float32)


def per_device(amplitudes, factors, occ_energy, virt_energy):
    z, upper, lower, x, core = position()
    rows, width = factors.shape
    half = width // 2
    pair_energy = (virt_energy[None, :] - occ_energy[:, None]).reshape(-1)
    energy_grid = pair_energy.reshape(8, 16, rows)
    row_energy = lax.dynamic_index_in_dim(energy_grid, z * 2 + upper, 0, keepdims=False)
    column_energy = lax.dynamic_index_in_dim(
        energy_grid, lower * 8 + x * 2 + core, 1, keepdims=False
    )

    band = gather_ring(factors[:, :half], "dx", 1)
    column_set = gather_ring(factors[:, half:], "dz", 2)
    band += swap_cores(band)
    far_low, far_high, near = transposed_product(amplitudes, band)
    leaving, keeping = straight_product(amplitudes, column_set)
    first = reduce_ring(
        far_low,
        far_high,
        near[: 2 * rows],
        near[2 * rows : 4 * rows],
        near[4 * rows :],
        "dz",
        2,
        upper == 1,
    )
    joined = keeping + send(leaving, core_flip=1).astype(jnp.float32)
    second = reduce_ring(
        joined[4 * rows : 5 * rows].astype(jnp.bfloat16),
        joined[5 * rows : 6 * rows].astype(jnp.bfloat16),
        joined[: 2 * rows],
        joined[2 * rows : 4 * rows],
        joined[6 * rows :],
        "dx",
        1,
        lower == 1,
    )
    images = factors.astype(jnp.float32) + jnp.concatenate([first, second], 1)
    dressed = images.astype(jnp.bfloat16)
    band = gather_ring(dressed, "dx", 1)
    column_set = gather_ring(dressed, "dz", 2)
    band += swap_cores(band)
    return outer_product(band, column_set, row_energy.reshape(-1), column_energy.reshape(-1))


def solution(mesh):
    placed = (P(AXIS, None, None), P(AXIS, None), P(), P())
    return jax.shard_map(
        per_device, mesh=mesh, in_specs=placed, out_specs=P(AXIS, None, None), check_vma=False
    )
```
